32 devices in a mesh: dp: 4 (over x, y), tp: 8 (over z, core).
Axes of the slice: x: 2, y: 2, z: 4, core: 2. Of those that a mesh axis runs over, the one named last changes fastest.
Arguments:
- x: bfloat16 [8192, 2048], P('dp'), parts along dimension 0
- dy: bfloat16 [8192, 2048], P('dp'), parts along dimension 0
- gate: bfloat16 [8192, 6144], P('dp', 'tp'), parts along dimension 0
- up: bfloat16 [8192, 6144], P('dp', 'tp'), parts along dimension 0
- w_gate: bfloat16 [2048, 6144], P(None, 'tp')
- w_up: bfloat16 [2048, 6144], P(None, 'tp')
- w_down: bfloat16 [6144, 2048], P('tp')
Outputs:
- output 1: bfloat16 [8192, 2048], P('dp'), parts along dimension 0
- output 2: bfloat16 [8192, 6144], P('dp', 'tp'), parts along dimension 0
- output 3: bfloat16 [8192, 6144], P('dp', 'tp'), parts along dimension 0
- output 4: bfloat16 [24576, 2048], P(('dp', 'tp')), parts along dimension 0
There are 4 independent parts. The reference program is written for one: setup_inputs(seed, part) draws one part's arguments, and reference() takes and returns one part's arrays. A program takes and returns all parts, laid end to end along the dimension named above; an argument that names none is the same for every part.
All inputs are finite; a program needn't handle non-finite values.
Results may differ from the reference program's by a relative error of at most 0.012.
Values are sent between devices in bfloat16 or wider.
A program may use at most 2 GiB of HBM per device.

```python
import jax
import jax.numpy as jnp

ROWS = 2048
D = 2048
FF = 6144


def act(gate, up):
    return jax.nn.silu(gate) * up


def setup_inputs(seed: int = 0, part: int = 0) -> dict:
    kx, ky, ka, kb, kg, ku, kd = jax.random.split(jax.random.key(seed), 7)
    kx, ky, ka, kb = (jax.random.fold_in(k, part) for k in (kx, ky, ka, kb))
    drawn = {
        "x": jax.random.normal(kx, (ROWS, D), jnp.float32),
        "dy": jax.random.normal(ky, (ROWS, D), jnp.float32),
        "gate": jax.random.normal(ka, (ROWS, FF), jnp.float32),
        "up": jax.random.normal(kb, (ROWS, FF), jnp.float32),
        "w_gate": jax.random.normal(kg, (D, FF), jnp.float32) * D**-0.5,
        "w_up": jax.random.normal(ku, (D, FF), jnp.float32) * D**-0.5,
        "w_down": jax.random.normal(kd, (FF, D), jnp.float32) * FF**-0.5,
    }
    return {k: v.astype(jnp.bfloat16) for k, v in drawn.items()}


def reference(x, dy, gate, up, w_gate, w_up, w_down):
    hidden, back = jax.vjp(act, gate.astype(jnp.float32), up.astype(jnp.float32))
    d_hidden = jnp.dot(dy, w_down.T, preferred_element_type=jnp.float32)
    d_gate, d_up = (g.astype(jnp.bfloat16) for g in back(d_hidden))
    dx = jnp.dot(d_gate, w_gate.T, preferred_element_type=jnp.float32) + jnp.dot(d_up, w_up.T, preferred_element_type=jnp.float32)
    dw_gate = jnp.dot(x.T, d_gate, preferred_element_type=jnp.float32)
    dw_up = jnp.dot(x.T, d_up, preferred_element_type=jnp.float32)
    dw_down = jnp.dot(hidden.astype(jnp.bfloat16).T, dy, preferred_element_type=jnp.float32)
    return tuple(g.astype(jnp.bfloat16) for g in (dx, dw_gate, dw_up, dw_down))
```

```python
import functools

import jax
import jax.numpy as jnp
from jax import lax
from jax.experimental import pallas as pl
from jax.experimental.pallas import tpu as pltpu
from jax.sharding import PartitionSpec as P

MESH = pl.DeviceIdType.MESH
F32, BF16 = jnp.float32, jnp.bfloat16

ROWS, D, FF = 2048, 2048, 768
RB = 256
CB = 256
HALF = D // 2
NB = ROWS // RB
NC = HALF // CB
CHUNKS = NB * NC
SUB = 2
PIECES = CHUNKS * SUB
PR_ROWS = RB // SUB
SLOTS = 4
HP = FF // 256
LAG_P, LAG_F, LAG_G = 3, 6, 9

NT = (((1,), (1,)), ((), ()))
TN = (((0,), (0,)), ((), ()))


def dot(a, b, dims):
    return lax.dot_general(a, b, dims, preferred_element_type=F32)


def ds(i, n):
    return pl.ds(pl.multiple_of(i * n, n), n)


def kernel(
    x, dy, gate, up, w_gate, w_up, w_down,
    dx, dwg, dwu, dwd,
    dyv, dg, du, hid, own, tb, pr, stage, gv, uv, xv,
    s_dy, s_g, s_u, s_w, s_wd, s_x, s_bs, s_br, s_t, s_in, s_pin, s_f, s_gs, s_gr,
):
    dp, me = lax.axis_index("dp"), lax.axis_index("tp")
    z, c = me // 2, me % 2
    sib = z * 2 + 1 - c
    edge = jnp.logical_or(z == 0, z == 3)
    mid = jnp.logical_not(edge)
    pair = (z + 1 - 2 * (z % 2)) * 2 + c
    across = (3 - z) * 2 + c
    col0 = c * HALF
    sibcol0 = (1 - c) * HALF

    barrier = pltpu.get_barrier_semaphore()
    for d in (sib, pair):
        pl.semaphore_signal(barrier, inc=1, device_id=(dp, d), device_id_type=MESH)

    @pl.when(mid)
    def _():
        pl.semaphore_signal(barrier, inc=1, device_id=(dp, across), device_id_type=MESH)

    def load_dy(b):
        return pltpu.make_async_copy(dy.at[ds(b, RB)], dyv.at[ds(b, RB)], s_dy.at[b])

    def load_g(b):
        return pltpu.make_async_copy(gate.at[ds(b, RB)], gv.at[b % 2], s_g.at[b % 2])

    def load_u(b):
        return pltpu.make_async_copy(up.at[ds(b, RB)], uv.at[b % 2], s_u.at[b % 2])

    def load_wd(h):
        return pltpu.make_async_copy(w_down.at[ds(h, 256)], dwd.at[ds(h, 256)], s_wd.at[h])

    def load_wg(p):
        return pltpu.make_async_copy(w_gate.at[ds(p, CB)], dwg.at[ds(p, CB)], s_w.at[0, p])

    def load_wu(p):
        return pltpu.make_async_copy(w_up.at[ds(p, CB)], dwu.at[ds(p, CB)], s_w.at[1, p])

    def load_x(t):
        return pltpu.make_async_copy(x.at[:, ds(t, 256)], xv.at[t % 2], s_x.at[t % 2])

    load_dy(0).start()
    load_wd(0).start()
    load_g(0).start()
    load_u(0).start()
    for h in range(1, HP):
        load_wd(h).start()
    for n in range(NC):
        for q in ((1 - c) * NC + n, c * NC + n):
            load_wg(q).start()
            load_wu(q).start()
    load_g(1).start()
    load_u(1).start()
    for b in range(1, NB):
        load_dy(b).start()
    load_x(0).start()
    load_x(1).start()

    def d_part(b, h):
        rows, cols = ds(b, RB), ds(h, 256)
        d_hidden = dot(dyv[rows, :], dwd[cols, :], NT)
        g = gv[b % 2, :, cols].astype(F32)
        u = uv[b % 2, :, cols].astype(F32)
        sig = jax.nn.sigmoid(g)
        act = g * sig
        hid[rows, cols] = (act * u).astype(BF16)
        du[rows, cols] = (d_hidden * act).astype(BF16)
        dg[rows, cols] = (d_hidden * u * (sig + act * (1.0 - sig))).astype(BF16)

    def term(b, q):
        rows, cols = ds(b, RB), ds(q, CB)
        return dot(dg[rows, :], dwg[cols, :], NT) + dot(du[rows, :], dwu[cols, :], NT)

    def to_sib(k):
        b, n = k // NC, k % NC
        dst = dx.at[ds(b, RB), ds((1 - c) * NC + n, CB)]
        return pltpu.make_async_remote_copy(
            stage.at[k % SLOTS], dst, s_bs.at[k % SLOTS], s_br.at[k], (dp, sib), MESH
        )

    def spot(s, half):
        k, h = s // SUB, s % SUB
        b, n = k // NC, k % NC
        return ds(b * SUB + h, PR_ROWS), ds(half * NC + n, CB)

    def to_mid(s):
        return pltpu.make_async_remote_copy(tb.at[s], tb.at[s], s_t, s_in.at[s], (dp, pair), MESH)

    def to_across(s):
        return pltpu.make_async_remote_copy(tb.at[s], pr.at[s], s_t, s_pin.at[s], (dp, across), MESH)

    def to_edge(s):
        ref = dx.at[spot(s, c)]
        return pltpu.make_async_remote_copy(ref, ref, s_f, s_in.at[s], (dp, pair), MESH)

    def final_to_sib(s):
        ref = dx.at[spot(s, c)]
        return pltpu.make_async_remote_copy(ref, ref, s_gs, s_gr, (dp, sib), MESH)

    def serve_a(k):
        to_sib(k).wait_recv()
        b, n = k // NC, k % NC
        total = own[k] + dx[ds(b, RB), ds(c * NC + n, CB)].astype(F32)

        @pl.when(edge)
        def _():
            for h in range(SUB):
                s = k * SUB + h
                tb[s] = total[h * PR_ROWS : (h + 1) * PR_ROWS].astype(BF16)
            for h in range(SUB):
                to_mid(k * SUB + h).start()

        @pl.when(mid)
        def _():
            own[k] = total

    def serve_p(s):
        @pl.when(mid)
        def _():
            to_mid(s).wait_recv()
            k, h = s // SUB, s % SUB
            tb[s] = (own[k, ds(h, PR_ROWS), :] + tb[s].astype(F32)).astype(BF16)
            to_across(s).start()

    def serve_f(s):
        @pl.when(mid)
        def _():
            to_across(s).wait_recv()
            dx[spot(s, c)] = (tb[s].astype(F32) + pr[s].astype(F32)).astype(BF16)
            to_edge(s).start()
            final_to_sib(s).start()

    def serve_g(s):
        @pl.when(edge)
        def _():
            to_edge(s).wait_recv()
            final_to_sib(s).start()

    def serve(i):
        for lag, f in ((LAG_P, serve_p), (LAG_F, serve_f), (LAG_G, serve_g)):
            s = i - lag
            pl.when(jnp.logical_and(s >= 0, s < PIECES))(functools.partial(f, s))

    def serve_all(i):
        serve_p(i - LAG_P)
        serve_f(i - LAG_F)
        serve_g(i - LAG_G)

    load_dy(0).wait()
    load_g(0).wait()
    load_u(0).wait()
    for h in range(HP):
        load_wd(h).wait()
        d_part(0, h)
    load_g(2).start()
    load_u(2).start()

    @pl.when(edge)
    def _():
        pl.semaphore_wait(barrier, 2)

    @pl.when(mid)
    def _():
        pl.semaphore_wait(barrier, 3)

    def step1(i, _):
        b, n = i // NC, i % NC
        qs, qo = (1 - c) * NC + n, c * NC + n

        @pl.when(b == 0)
        def _():
            load_wg(qs).wait()
            load_wu(qs).wait()

        @pl.when(i >= SLOTS)
        def _():
            to_sib(i - SLOTS).wait_send()

        stage[i % SLOTS] = term(b, qs).astype(BF16)
        to_sib(i).start()

        @pl.when(i >= 1)
        def _():
            serve_a(i - 1)

        @pl.when(b == 0)
        def _():
            load_wg(qo).wait()
            load_wu(qo).wait()

        own[i] = term(b, qo)
        serve(i)

        @pl.when(jnp.logical_and(n == 0, b < NB - 1))
        def _():
            load_dy(b + 1).wait()
            load_g(b + 1).wait()
            load_u(b + 1).wait()

        @pl.when(jnp.logical_and(n < HP, b < NB - 1))
        def _():
            d_part(b + 1, n)

        @pl.when(jnp.logical_and(n == NC - 1, b < NB - 3))
        def _():
            load_g(b + 3).start()
            load_u(b + 3).start()

        return 0

    lax.fori_loop(0, CHUNKS, step1, 0)
    serve_a(CHUNKS - 1)

    def step2(t, _):
        load_x(t).wait()
        rows = ds(t, 256)
        dwg[rows, :] = dot(xv[t % 2], dg[...], TN).astype(BF16)
        serve_all(CHUNKS + 2 * t)
        dwu[rows, :] = dot(xv[t % 2], du[...], TN).astype(BF16)

        @pl.when(t < D // 256 - 2)
        def _():
            load_x(t + 2).start()

        serve_all(CHUNKS + 2 * t + 1)
        return 0

    lax.fori_loop(0, D // 256, step2, 0)
    base = CHUNKS + 2 * (D // 256)

    def step3(i, _):
        rows, cols = ds(i // 4, 256), ds(i % 4, 512)
        dwd[rows, cols] = dot(hid[:, rows], dyv[:, cols], TN).astype(BF16)
        serve_all(base + i)
        return 0

    lax.fori_loop(0, HP * 4, step3, 0)
    base = base + HP * 4

    def step4(i, _):
        serve(i)
        return 0

    lax.fori_loop(base, PIECES + LAG_G, step4, 0)

    for k in range(SLOTS):
        to_sib(CHUNKS - SLOTS + k).wait_send()
    other = dx.at[:, ds(1 - c, HALF)]
    mine = dx.at[:, ds(c, HALF)]
    pltpu.make_async_copy(tb, tb, s_t).wait()
    pltpu.make_async_copy(mine, mine, s_gs).wait()
    pltpu.make_async_copy(other, other, s_gr).wait()

    @pl.when(mid)
    def _():
        pltpu.make_async_copy(mine, mine, s_f).wait()


def writer(a, b, c, d, oa, ob, oc, od, sems):
    copies = [pltpu.make_async_copy(s, t, sems.at[i]) for i, (s, t) in enumerate(((a, oa), (b, ob), (c, oc), (d, od)))]
    for copy in copies:
        copy.start()
    for copy in copies:
        copy.wait()


def solution(mesh):
    shapes = ((ROWS, D), (D, FF), (D, FF), (FF, D))

    def step(*args):
        dma = pltpu.SemaphoreType.DMA
        parts = pl.pallas_call(
            kernel,
            out_shape=[pltpu.VMEM(s, BF16) for s in shapes],
            in_specs=[pl.BlockSpec(memory_space=pl.ANY)] * 7,
            out_specs=[pl.BlockSpec(memory_space=pltpu.VMEM)] * 4,
            scratch_shapes=[
                pltpu.VMEM((ROWS, D), BF16),
                pltpu.VMEM((ROWS, FF), BF16),
                pltpu.VMEM((ROWS, FF), BF16),
                pltpu.VMEM((ROWS, FF), BF16),
                pltpu.VMEM((CHUNKS, RB, CB), F32),
                pltpu.VMEM((PIECES, PR_ROWS, CB), BF16),
                pltpu.VMEM((PIECES, PR_ROWS, CB), BF16),
                pltpu.VMEM((SLOTS, RB, CB), BF16),
                pltpu.VMEM((2, RB, FF), BF16),
                pltpu.VMEM((2, RB, FF), BF16),
                pltpu.VMEM((2, ROWS, 256), BF16),
                dma((NB,)),
                dma((2,)),
                dma((2,)),
                dma((2, 2 * NC)),
                dma((HP,)),
                dma((2,)),
                dma((SLOTS,)),
                dma((CHUNKS,)),
                dma,
                dma((PIECES,)),
                dma((PIECES,)),
                dma,
                dma,
                dma,
            ],
            compiler_params=pltpu.CompilerParams(
                collective_id=0, has_side_effects=True, vmem_limit_bytes=44 * 1024 * 1024
            ),
        )(*args)
        return pl.pallas_call(
            writer,
            out_shape=[jax.ShapeDtypeStruct(s, BF16) for s in shapes],
            in_specs=[pl.BlockSpec(memory_space=pltpu.VMEM)] * 4,
            out_specs=[pl.BlockSpec(memory_space=pl.ANY)] * 4,
            scratch_shapes=[pltpu.SemaphoreType.DMA((4,))],
            compiler_params=pltpu.CompilerParams(vmem_limit_bytes=1024 * 1024),
        )(*parts)

    tokens, columns, rows = P("dp", None), P(None, "tp"), P("tp", None)
    return jax.shard_map(
        step,
        mesh=mesh,
        in_specs=(tokens, tokens, P("dp", "tp"), P("dp", "tp"), columns, columns, rows),
        out_specs=(tokens, P("dp", "tp"), P("dp", "tp"), P(("dp", "tp"), None)),
        check_vma=False,
    )
```

```python
import functools

import jax
import jax.numpy as jnp
from jax import lax
from jax.experimental import pallas as pl
from jax.experimental.pallas import tpu as pltpu
from jax.sharding import PartitionSpec as P

MESH = pl.DeviceIdType.MESH
F32, BF16 = jnp.float32, jnp.bfloat16

ROWS, D, FF = 2048, 2048, 768
RB = 256
CB = 256
HALF = D // 2
NB = ROWS // RB
NC = HALF // CB
CHUNKS = NB * NC
SUB = 2
PIECES = CHUNKS * SUB
PR_ROWS = RB // SUB
SLOTS = 4
HP = FF // 256
LAG_P, LAG_F, LAG_G = 3, 6, 9
PER_BLOCK = NC + 1

NT = (((1,), (1,)), ((), ()))
TN = (((0,), (0,)), ((), ()))


def dot(a, b, dims):
    return lax.dot_general(a, b, dims, preferred_element_type=F32)


def div(a, n):
    return lax.div(a, jnp.int32(n)) if isinstance(a, jax.Array) else a // n


def rem(a, n):
    return lax.rem(a, jnp.int32(n)) if isinstance(a, jax.Array) else a % n


def ds(i, n):
    return pl.ds(pl.multiple_of(i * n, n), n)


def kernel(
    x, dy, gate, up, w_gate, w_up, w_down,
    dx, dwg, dwu, dwd,
    dyv, dgu, hid, own, tb, pr, stage, gv, uv, xv,
    s_dy, s_g, s_u, s_w, s_wd, s_x, s_bs, s_br, s_t, s_in, s_pin, s_f, s_gs, s_gr,
):
    dp, me = lax.axis_index("dp"), lax.axis_index("tp")
    z, c = div(me, 2), rem(me, 2)
    sib = z * 2 + 1 - c
    edge = jnp.logical_or(z == 0, z == 3)
    mid = jnp.logical_not(edge)
    pair = (z + 1 - 2 * rem(z, 2)) * 2 + c
    across = (3 - z) * 2 + c
    col0 = c * HALF
    sibcol0 = (1 - c) * HALF

    barrier = pltpu.get_barrier_semaphore()
    for d in (sib, pair):
        pl.semaphore_signal(barrier, inc=1, device_id=(dp, d), device_id_type=MESH)

    @pl.when(mid)
    def _():
        pl.semaphore_signal(barrier, inc=1, device_id=(dp, across), device_id_type=MESH)

    def load_dy(b):
        return pltpu.make_async_copy(dy.at[ds(b, RB)], dyv.at[ds(b, RB)], s_dy.at[b])

    def load_g(b):
        return pltpu.make_async_copy(gate.at[ds(b, RB)], gv.at[rem(b, 2)], s_g.at[rem(b, 2)])

    def load_u(b):
        return pltpu.make_async_copy(up.at[ds(b, RB)], uv.at[rem(b, 2)], s_u.at[rem(b, 2)])

    def load_wd(h):
        return pltpu.make_async_copy(w_down.at[ds(h, 256)], dwd.at[ds(h, 256)], s_wd.at[h])

    def load_wg(p):
        return pltpu.make_async_copy(w_gate.at[ds(p, CB)], dwg.at[ds(p, CB)], s_w.at[0, p])

    def load_wu(p):
        return pltpu.make_async_copy(w_up.at[ds(p, CB)], dwu.at[ds(p, CB)], s_w.at[1, p])

    def load_x(t):
        return pltpu.make_async_copy(x.at[:, ds(t, 256)], xv.at[rem(t, 2)], s_x.at[rem(t, 2)])

    def load_w(n):
        for q in ((1 - c) * NC + n, c * NC + n):
            load_wg(q).start()
            load_wu(q).start()

    def load_rows(b):
        load_dy(b).start()
        load_g(b).start()
        load_u(b).start()

    load_wd(0).start()
    load_rows(0)
    load_wd(1).start()
    load_wd(2).start()
    load_w(0)

    def d_part(b, h):
        rows, cols = ds(b, RB), ds(h, 256)
        d_hidden = dot(dyv[rows, :], dwd[cols, :], NT)
        g = gv[rem(b, 2), :, cols].astype(F32)
        u = uv[rem(b, 2), :, cols].astype(F32)
        sig = jax.nn.sigmoid(g)
        act = g * sig
        hid[rows, cols] = (act * u).astype(BF16)
        dgu[rows, ds(HP + h, 256)] = (d_hidden * act).astype(BF16)
        dgu[rows, cols] = (d_hidden * u * (sig + act * (1.0 - sig))).astype(BF16)

    def term(b, q):
        rows, cols = ds(b, RB), ds(q, CB)
        return dot(dgu[rows, :FF], dwg[cols, :], NT) + dot(dgu[rows, FF:], dwu[cols, :], NT)

    def to_sib(k):
        b, n = div(k, NC), rem(k, NC)
        dst = dx.at[ds(b, RB), ds((1 - c) * NC + n, CB)]
        return pltpu.make_async_remote_copy(
            stage.at[rem(k, SLOTS)], dst, s_bs.at[rem(k, SLOTS)], s_br.at[k], (dp, sib), MESH
        )

    def spot(s, half):
        k, h = div(s, SUB), rem(s, SUB)
        b, n = div(k, NC), rem(k, NC)
        return ds(b * SUB + h, PR_ROWS), ds(half * NC + n, CB)

    def to_mid(s):
        return pltpu.make_async_remote_copy(tb.at[s], tb.at[s], s_t, s_in.at[s], (dp, pair), MESH)

    def to_across(s):
        return pltpu.make_async_remote_copy(tb.at[s], pr.at[s], s_t, s_pin.at[s], (dp, across), MESH)

    def to_edge(s):
        ref = dx.at[spot(s, c)]
        return pltpu.make_async_remote_copy(ref, ref, s_f, s_in.at[s], (dp, pair), MESH)

    def final_to_sib(s):
        ref = dx.at[spot(s, c)]
        return pltpu.make_async_remote_copy(ref, ref, s_gs, s_gr, (dp, sib), MESH)

    def serve_a(k):
        to_sib(k).wait_recv()
        b, n = div(k, NC), rem(k, NC)
        total = own[k] + dx[ds(b, RB), ds(c * NC + n, CB)].astype(F32)

        @pl.when(edge)
        def _():
            for h in range(SUB):
                s = k * SUB + h
                tb[s] = total[h * PR_ROWS : (h + 1) * PR_ROWS].astype(BF16)
            for h in range(SUB):
                to_mid(k * SUB + h).start()

        @pl.when(mid)
        def _():
            own[k] = total

    def serve_p(s):
        @pl.when(mid)
        def _():
            to_mid(s).wait_recv()
            k, h = div(s, SUB), rem(s, SUB)
            tb[s] = (own[k, ds(h, PR_ROWS), :] + tb[s].astype(F32)).astype(BF16)
            to_across(s).start()

    def serve_f(s):
        @pl.when(mid)
        def _():
            to_across(s).wait_recv()
            dx[spot(s, c)] = (tb[s].astype(F32) + pr[s].astype(F32)).astype(BF16)
            to_edge(s).start()
            final_to_sib(s).start()

    def serve_g(s):
        @pl.when(edge)
        def _():
            to_edge(s).wait_recv()
            final_to_sib(s).start()

    def serve(i):
        for lag, f in ((LAG_P, serve_p), (LAG_F, serve_f), (LAG_G, serve_g)):
            s = i - lag
            pl.when(jnp.logical_and(s >= 0, s < PIECES))(functools.partial(f, s))

    load_dy(0).wait()
    load_g(0).wait()
    load_u(0).wait()
    for h in range(HP):
        load_wd(h).wait()
        if h == HP - 1:
            for n in range(1, NC):
                load_w(n)
            load_rows(1)
        d_part(0, h)

    @pl.when(edge)
    def _():
        pl.semaphore_wait(barrier, 2)

    @pl.when(mid)
    def _():
        pl.semaphore_wait(barrier, 3)

    def step1(i, _):
        b, n = div(i, NC), rem(i, NC)
        qs, qo = (1 - c) * NC + n, c * NC + n

        @pl.when(b == 0)
        def _():
            for q in (qs, qo):
                load_wg(q).wait()
                load_wu(q).wait()

        @pl.when(i >= SLOTS)
        def _():
            to_sib(i - SLOTS).wait_send()

        theirs, ours = term(b, qs), term(b, qo)
        stage[rem(i, SLOTS)] = theirs.astype(BF16)
        own[i] = ours
        to_sib(i).start()

        @pl.when(i >= 1)
        def _():
            serve_a(i - 1)

        serve(b * PER_BLOCK + n)

        @pl.when(jnp.logical_and(n == 1, b < NB - 1))
        def _():
            load_dy(b + 1).wait()
            load_g(b + 1).wait()
            load_u(b + 1).wait()

            @pl.when(b < NB - 2)
            def _():
                load_rows(b + 2)

        @pl.when(jnp.logical_and(n >= 1, b < NB - 1))
        def _():
            d_part(b + 1, n - 1)

        pl.when(n == NC - 1)(functools.partial(serve, b * PER_BLOCK + NC))

        @pl.when(i == CHUNKS - 2)
        def _():
            load_x(0).start()
            load_x(1).start()

        return 0

    lax.fori_loop(0, CHUNKS, step1, 0)
    serve_a(CHUNKS - 1)

    def step2(t, _):
        load_x(t).wait()
        rows = ds(t, 256)
        for q in range(3):
            part = dot(xv[rem(t, 2)], dgu[:, q * 512 : (q + 1) * 512], TN).astype(BF16)
            if q == 0:
                dwg[rows, :512] = part
            elif q == 1:
                dwg[rows, 512:] = part[:, :256]
                dwu[rows, :256] = part[:, 256:]
            else:
                dwu[rows, 256:] = part

                @pl.when(t < D // 256 - 2)
                def _():
                    load_x(t + 2).start()

            if q > 0:
                serve(NB * PER_BLOCK + 2 * t + q - 1)
        return 0

    lax.fori_loop(0, D // 256, step2, 0)
    base = NB * PER_BLOCK + 2 * (D // 256)

    def step3(i, _):
        q, h = div(i, HP), rem(i, HP)
        rows, cols = ds(h, 256), ds(q, 512)
        dwd[rows, cols] = dot(hid[:, rows], dyv[:, cols], TN).astype(BF16)
        pl.when(h > 0)(functools.partial(serve, base + q * (HP - 1) + h - 1))
        return 0

    lax.fori_loop(0, HP * 4, step3, 0)
    base = base + (HP - 1) * 4

    def step4(i, _):
        serve(i)
        return 0

    lax.fori_loop(base, PIECES + LAG_G, step4, 0)

    for k in range(SLOTS):
        to_sib(CHUNKS - SLOTS + k).wait_send()
    other = dx.at[:, ds(1 - c, HALF)]
    mine = dx.at[:, ds(c, HALF)]
    pltpu.make_async_copy(tb, tb, s_t).wait()
    pltpu.make_async_copy(mine, mine, s_gs).wait()
    pltpu.make_async_copy(other, other, s_gr).wait()

    @pl.when(mid)
    def _():
        pltpu.make_async_copy(mine, mine, s_f).wait()


def writer(a, b, c, d, oa, ob, oc, od, sems):
    copies = [pltpu.make_async_copy(s, t, sems.at[i]) for i, (s, t) in enumerate(((a, oa), (b, ob), (c, oc), (d, od)))]
    for copy in copies:
        copy.start()
    for copy in copies:
        copy.wait()


def solution(mesh):
    shapes = ((ROWS, D), (D, FF), (D, FF), (FF, D))

    def step(*args):
        dma = pltpu.SemaphoreType.DMA
        parts = pl.pallas_call(
            kernel,
            out_shape=[pltpu.VMEM(s, BF16) for s in shapes],
            in_specs=[pl.BlockSpec(memory_space=pl.ANY)] * 7,
            out_specs=[pl.BlockSpec(memory_space=pltpu.VMEM)] * 4,
            scratch_shapes=[
                pltpu.VMEM((ROWS, D), BF16),
                pltpu.VMEM((ROWS, 2 * FF), BF16),
                pltpu.VMEM((ROWS, FF), BF16),
                pltpu.VMEM((CHUNKS, RB, CB), F32),
                pltpu.VMEM((PIECES, PR_ROWS, CB), BF16),
                pltpu.VMEM((PIECES, PR_ROWS, CB), BF16),
                pltpu.VMEM((SLOTS, RB, CB), BF16),
                pltpu.VMEM((2, RB, FF), BF16),
                pltpu.VMEM((2, RB, FF), BF16),
                pltpu.VMEM((2, ROWS, 256), BF16),
                dma((NB,)),
                dma((2,)),
                dma((2,)),
                dma((2, 2 * NC)),
                dma((HP,)),
                dma((2,)),
                dma((SLOTS,)),
                dma((CHUNKS,)),
                dma,
                dma((PIECES,)),
                dma((PIECES,)),
                dma,
                dma,
                dma,
            ],
            compiler_params=pltpu.CompilerParams(
                collective_id=0, has_side_effects=True, vmem_limit_bytes=44 * 1024 * 1024
            ),
        )(*args)
        return pl.pallas_call(
            writer,
            out_shape=[jax.ShapeDtypeStruct(s, BF16) for s in shapes],
            in_specs=[pl.BlockSpec(memory_space=pltpu.VMEM)] * 4,
            out_specs=[pl.BlockSpec(memory_space=pl.ANY)] * 4,
            scratch_shapes=[pltpu.SemaphoreType.DMA((4,))],
            compiler_params=pltpu.CompilerParams(vmem_limit_bytes=1024 * 1024),
        )(*parts)

    tokens, columns, rows = P("dp", None), P(None, "tp"), P("tp", None)
    return jax.shard_map(
        step,
        mesh=mesh,
        in_specs=(tokens, tokens, P("dp", "tp"), P("dp", "tp"), columns, columns, rows),
        out_specs=(tokens, P("dp", "tp"), P("dp", "tp"), P(("dp", "tp"), None)),
        check_vma=False,
    )
```

```python
import functools

import jax
import jax.numpy as jnp
from jax import lax
from jax.experimental import pallas as pl
from jax.experimental.pallas import tpu as pltpu
from jax.sharding import PartitionSpec as P

MESH = pl.DeviceIdType.MESH
F32, BF16 = jnp.float32, jnp.bfloat16

ROWS, D, FF = 2048, 2048, 768
RB = 256
CB = 512
NB = ROWS // RB
NC = D // CB
CHUNKS = NB * NC
SUB = 2
PIECES = CHUNKS * SUB
PR_ROWS = RB // SUB
SLOTS = 4
DEPTH = 16
HP = FF // 256
LAG_P, LAG_F, LAG_G = 4, 8, 12
PER_BLOCK = NC + 1

NT = (((1,), (1,)), ((), ()))
TN = (((0,), (0,)), ((), ()))


def dot(a, b, dims):
    return lax.dot_general(a, b, dims, preferred_element_type=F32)


def div(a, n):
    return lax.div(a, jnp.int32(n)) if isinstance(a, jax.Array) else a // n


def rem(a, n):
    return lax.rem(a, jnp.int32(n)) if isinstance(a, jax.Array) else a % n


def ds(i, n):
    return pl.ds(pl.multiple_of(i * n, n), n)


def kernel(
    x, dy, gate, up, w_gate, w_up, w_down,
    dx, dwg, dwu, dwd,
    dyv, dgu, hid, own, tb, stage, gv, uv, xv,
    s_dy, s_g, s_u, s_w, s_wd, s_x, s_bs, s_br, s_t, s_in, s_pl, s_f, s_gs, s_gr,
):
    dp, me = lax.axis_index("dp"), lax.axis_index("tp")
    z, c = div(me, 2), rem(me, 2)
    sib = z * 2 + 1 - c
    edge = jnp.logical_or(z == 0, z == 3)
    mid = jnp.logical_not(edge)
    pair = (z + 1 - 2 * rem(z, 2)) * 2 + c
    across = (3 - z) * 2 + 1 - c
    adds, ends = c == 1, c == 0

    def load_dy(b):
        return pltpu.make_async_copy(dy.at[ds(b, RB)], dyv.at[ds(b, RB)], s_dy.at[b])

    def load_g(b):
        return pltpu.make_async_copy(gate.at[ds(b, RB)], gv.at[rem(b, 2)], s_g.at[rem(b, 2)])

    def load_u(b):
        return pltpu.make_async_copy(up.at[ds(b, RB)], uv.at[rem(b, 2)], s_u.at[rem(b, 2)])

    def load_wd(h):
        return pltpu.make_async_copy(w_down.at[ds(h, 256)], dwd.at[ds(h, 256)], s_wd.at[h])

    def load_wg(p):
        return pltpu.make_async_copy(w_gate.at[ds(p, CB)], dwg.at[ds(p, CB)], s_w.at[0, p])

    def load_wu(p):
        return pltpu.make_async_copy(w_up.at[ds(p, CB)], dwu.at[ds(p, CB)], s_w.at[1, p])

    def load_x(t):
        return pltpu.make_async_copy(x.at[:, ds(t, 256)], xv.at[rem(t, 2)], s_x.at[rem(t, 2)])

    def load_w(n):
        load_wg(n).start()
        load_wu(n).start()

    def load_rows(b):
        load_dy(b).start()
        load_g(b).start()
        load_u(b).start()

    load_wd(0).start()
    load_rows(0)
    load_wd(1).start()
    load_wd(2).start()
    load_w(0)

    barrier = pltpu.get_barrier_semaphore()
    for d in (sib, pair):
        pl.semaphore_signal(barrier, inc=1, device_id=(dp, d), device_id_type=MESH)

    @pl.when(mid)
    def _():
        pl.semaphore_signal(barrier, inc=1, device_id=(dp, across), device_id_type=MESH)


    def d_part(b, h):
        rows, cols = ds(b, RB), ds(h, 256)
        d_hidden = dot(dyv[rows, :], dwd[cols, :], NT)
        g = gv[rem(b, 2), :, cols].astype(F32)
        u = uv[rem(b, 2), :, cols].astype(F32)
        sig = jax.nn.sigmoid(g)
        act = g * sig
        hid[rows, cols] = (act * u).astype(BF16)
        dgu[rows, ds(HP + h, 256)] = (d_hidden * act).astype(BF16)
        dgu[rows, cols] = (d_hidden * u * (sig + act * (1.0 - sig))).astype(BF16)

    def term(k):
        rows, cols = ds(div(k, NC), RB), ds(rem(k, NC), CB)
        return dot(dgu[rows, :FF], dwg[cols, :], NT) + dot(dgu[rows, FF:], dwu[cols, :], NT)

    def remote(src, dst, send, recv, device):
        return pltpu.make_async_remote_copy(src, dst, send, recv, (dp, device), MESH)

    def tile(k):
        return ds(div(k, NC), RB), ds(rem(k, NC), CB)

    def spot(s):
        k, h = div(s, SUB), rem(s, SUB)
        return ds(div(k, NC) * SUB + h, PR_ROWS), ds(rem(k, NC), CB)

    def to_sib(k):
        q = rem(k, SLOTS)
        return remote(stage.at[q], dx.at[tile(k)], s_bs.at[q], s_br.at[k], sib)

    def to_mid(s):
        return remote(tb.at[s], tb.at[s], s_t, s_in.at[s], pair)

    def to_across(s):
        return remote(tb.at[s], tb.at[s], s_t, s_in.at[s], across)

    def part_to_sib(s):
        return remote(tb.at[s], dx.at[spot(s)], s_gs, s_pl.at[s], sib)

    def to_edge(s):
        ref = dx.at[spot(s)]
        return remote(ref, ref, s_f, s_in.at[s], pair)

    def final_to_sib(s):
        ref = dx.at[spot(s)]
        return remote(ref, ref, s_gs, s_gr, sib)

    def both(a, b):
        return pl.when(jnp.logical_and(a, b))

    def serve_a(k):
        @pl.when(adds)
        def _():
            to_sib(k).wait_recv()

        def total(h):
            rows, cols = spot(k * SUB + h)
            return own[rem(k, DEPTH), pl.ds(h * PR_ROWS, PR_ROWS), :] + dx[rows, cols].astype(F32)

        @both(adds, edge)
        def _():
            for h in range(SUB):
                s = k * SUB + h
                tb[s] = total(h).astype(BF16)
                to_mid(s).start()

        @both(adds, mid)
        def _():
            for h in range(SUB):
                own[rem(k, DEPTH), pl.ds(h * PR_ROWS, PR_ROWS), :] = total(h)

    def serve_p(s):
        @both(adds, mid)
        def _():
            to_mid(s).wait_recv()
            k, h = div(s, SUB), rem(s, SUB)
            tb[s] = (own[rem(k, DEPTH), ds(h, PR_ROWS), :] + tb[s].astype(F32)).astype(BF16)
            to_across(s).start()
            part_to_sib(s).start()

    def serve_f(s):
        @both(ends, mid)
        def _():
            part_to_sib(s).wait_recv()
            to_across(s).wait_recv()
            rows, cols = spot(s)
            dx[rows, cols] = (dx[rows, cols].astype(F32) + tb[s].astype(F32)).astype(BF16)
            to_edge(s).start()
            final_to_sib(s).start()

    def serve_g(s):
        @both(ends, edge)
        def _():
            to_edge(s).wait_recv()
            final_to_sib(s).start()

    def serve(i):
        for lag, f in ((LAG_P, serve_p), (LAG_F, serve_f), (LAG_G, serve_g)):
            s = i - lag
            pl.when(jnp.logical_and(s >= 0, s < PIECES))(functools.partial(f, s))

    load_dy(0).wait()
    load_g(0).wait()
    load_u(0).wait()
    for h in range(HP):
        load_wd(h).wait()
        if h == HP - 1:
            for n in range(1, NC):
                load_w(n)
            load_rows(1)
        d_part(0, h)

    @pl.when(edge)
    def _():
        pl.semaphore_wait(barrier, 2)

    @pl.when(mid)
    def _():
        pl.semaphore_wait(barrier, 3)

    def step1(i, _):
        b, n = div(i, NC), rem(i, NC)

        @pl.when(b == 0)
        def _():
            load_wg(n).wait()
            load_wu(n).wait()

        @both(ends, i >= SLOTS)
        def _():
            to_sib(i - SLOTS).wait_send()

        t = term(i)
        own[rem(i, DEPTH)] = t
        stage[rem(i, SLOTS)] = t.astype(BF16)

        @pl.when(ends)
        def _():
            to_sib(i).start()

        @pl.when(i >= 1)
        def _():
            serve_a(i - 1)

        serve(b * PER_BLOCK + n)

        @pl.when(jnp.logical_and(n == 1, b < NB - 1))
        def _():
            load_dy(b + 1).wait()
            load_g(b + 1).wait()
            load_u(b + 1).wait()

            @pl.when(b < NB - 2)
            def _():
                load_rows(b + 2)

        @pl.when(jnp.logical_and(n >= 1, b < NB - 1))
        def _():
            d_part(b + 1, n - 1)

        pl.when(n == NC - 1)(functools.partial(serve, b * PER_BLOCK + NC))

        @pl.when(i == CHUNKS - 2)
        def _():
            load_x(0).start()
            load_x(1).start()

        return 0

    lax.fori_loop(0, CHUNKS, step1, 0)
    serve_a(CHUNKS - 1)

    def step2(t, _):
        load_x(t).wait()
        rows = ds(t, 256)
        for q in range(3):
            part = dot(xv[rem(t, 2)], dgu[:, q * 512 : (q + 1) * 512], TN).astype(BF16)
            if q == 0:
                dwg[rows, :512] = part
            elif q == 1:
                dwg[rows, 512:] = part[:, :256]
                dwu[rows, :256] = part[:, 256:]
            else:
                dwu[rows, 256:] = part

                @pl.when(t < D // 256 - 2)
                def _():
                    load_x(t + 2).start()

            if q > 0:
                serve(NB * PER_BLOCK + 2 * t + q - 1)
        return 0

    lax.fori_loop(0, D // 256, step2, 0)
    base = NB * PER_BLOCK + 2 * (D // 256)

    def step3(i, _):
        q, h = div(i, HP), rem(i, HP)
        rows, cols = ds(h, 256), ds(q, 512)
        dwd[rows, cols] = dot(hid[:, rows], dyv[:, cols], TN).astype(BF16)
        pl.when(h > 0)(functools.partial(serve, base + q * (HP - 1) + h - 1))
        return 0

    lax.fori_loop(0, HP * 4, step3, 0)
    base = base + (HP - 1) * 4

    def step4(i, _):
        serve(i)
        return 0

    lax.fori_loop(base, PIECES + LAG_G, step4, 0)

    @pl.when(adds)
    def _():
        pltpu.make_async_copy(tb, tb, s_t).wait()
        pltpu.make_async_copy(dx, dx, s_gr).wait()

    @both(adds, mid)
    def _():
        pltpu.make_async_copy(tb, tb, s_gs).wait()

    @pl.when(ends)
    def _():
        for k in range(SLOTS):
            to_sib(CHUNKS - SLOTS + k).wait_send()
        pltpu.make_async_copy(dx, dx, s_gs).wait()

    @both(ends, mid)
    def _():
        pltpu.make_async_copy(dx, dx, s_f).wait()


def writer(a, b, c, d, oa, ob, oc, od, sems):
    copies = []
    for i, (src, dst) in enumerate(((a, oa), (b, ob), (c, oc), (d, od))):
        for k in range(4):
            rows = pl.ds(k * (src.shape[0] // 4), src.shape[0] // 4)
            copies.append(pltpu.make_async_copy(src.at[rows], dst.at[rows], sems.at[i, k]))
    for copy in copies:
        copy.start()
    for copy in copies:
        copy.wait()


def solution(mesh):
    shapes = ((ROWS, D), (D, FF), (D, FF), (FF, D))

    def step(*args):
        dma = pltpu.SemaphoreType.DMA
        parts = pl.pallas_call(
            kernel,
            out_shape=[pltpu.VMEM(s, BF16) for s in shapes],
            in_specs=[pl.BlockSpec(memory_space=pl.ANY)] * 7,
            out_specs=[pl.BlockSpec(memory_space=pltpu.VMEM)] * 4,
            scratch_shapes=[
                pltpu.VMEM((ROWS, D), BF16),
                pltpu.VMEM((ROWS, 2 * FF), BF16),
                pltpu.VMEM((ROWS, FF), BF16),
                pltpu.VMEM((DEPTH, RB, CB), F32),
                pltpu.VMEM((PIECES, PR_ROWS, CB), BF16),
                pltpu.VMEM((SLOTS, RB, CB), BF16),
                pltpu.VMEM((2, RB, FF), BF16),
                pltpu.VMEM((2, RB, FF), BF16),
                pltpu.VMEM((2, ROWS, 256), BF16),
                dma((NB,)),
                dma((2,)),
                dma((2,)),
                dma((2, NC)),
                dma((HP,)),
                dma((2,)),
                dma((SLOTS,)),
                dma((CHUNKS,)),
                dma,
                dma((PIECES,)),
                dma((PIECES,)),
                dma,
                dma,
                dma,
            ],
            compiler_params=pltpu.CompilerParams(
                collective_id=0, has_side_effects=True, vmem_limit_bytes=44 * 1024 * 1024
            ),
        )(*args)
        return pl.pallas_call(
            writer,
            out_shape=[jax.ShapeDtypeStruct(s, BF16) for s in shapes],
            in_specs=[pl.BlockSpec(memory_space=pltpu.VMEM)] * 4,
            out_specs=[pl.BlockSpec(memory_space=pl.ANY)] * 4,
            scratch_shapes=[pltpu.SemaphoreType.DMA((4, 4))],
            compiler_params=pltpu.CompilerParams(vmem_limit_bytes=1024 * 1024),
        )(*parts)

    tokens, columns, rows = P("dp", None), P(None, "tp"), P("tp", None)
    return jax.shard_map(
        step,
        mesh=mesh,
        in_specs=(tokens, tokens, P("dp", "tp"), P("dp", "tp"), columns, columns, rows),
        out_specs=(tokens, P("dp", "tp"), P("dp", "tp"), P(("dp", "tp"), None)),
        check_vma=False,
    )
```

```python
import functools

import jax
import jax.numpy as jnp
from jax import lax
from jax.experimental import pallas as pl
from jax.experimental.pallas import tpu as pltpu
from jax.sharding import PartitionSpec as P

MESH = pl.DeviceIdType.MESH
F32, BF16 = jnp.float32, jnp.bfloat16

ROWS, D, FF = 2048, 2048, 768
RB = 256
CB = 512
NB = ROWS // RB
NC = D // CB
CHUNKS = NB * NC
SUB = 2
PIECES = CHUNKS * SUB
PR_ROWS = RB // SUB
SLOTS = 4
DEPTH = 16
HP = FF // 256
LAG_P, LAG_F, LAG_G = 5, 9, 14
PER_BLOCK = NC + 1

NT = (((1,), (1,)), ((), ()))
TN = (((0,), (0,)), ((), ()))


def dot(a, b, dims):
    return lax.dot_general(a, b, dims, preferred_element_type=F32)


def div(a, n):
    return lax.div(a, jnp.int32(n)) if isinstance(a, jax.Array) else a // n


def rem(a, n):
    return lax.rem(a, jnp.int32(n)) if isinstance(a, jax.Array) else a % n


def ds(i, n):
    return pl.ds(pl.multiple_of(i * n, n), n)


def kernel(
    x, dy, gate, up, w_gate, w_up, w_down,
    dx, dwg, dwu, dwd,
    dyv, dgu, hid, own, tb, stage, gv, uv, xv,
    s_dy, s_g, s_u, s_w, s_wd, s_x, s_bs, s_br, s_t, s_in, s_pl, s_f, s_gs, s_gr,
):
    dp, me = lax.axis_index("dp"), lax.axis_index("tp")
    z, c = div(me, 2), rem(me, 2)
    sib = z * 2 + 1 - c
    edge = jnp.logical_or(z == 0, z == 3)
    mid = jnp.logical_not(edge)
    pair = (z + 1 - 2 * rem(z, 2)) * 2 + c
    across = (3 - z) * 2 + 1 - c
    adds, ends = c == 1, c == 0

    def load_dy(b):
        return pltpu.make_async_copy(dy.at[ds(b, RB)], dyv.at[ds(b, RB)], s_dy.at[b])

    def load_g(b):
        return pltpu.make_async_copy(gate.at[ds(b, RB)], gv.at[rem(b, 2)], s_g.at[rem(b, 2)])

    def load_u(b):
        return pltpu.make_async_copy(up.at[ds(b, RB)], uv.at[rem(b, 2)], s_u.at[rem(b, 2)])

    def load_wd(h):
        return pltpu.make_async_copy(w_down.at[ds(h, 256)], dwd.at[ds(h, 256)], s_wd.at[h])

    def load_wg(p):
        return pltpu.make_async_copy(w_gate.at[ds(p, CB)], dwg.at[ds(p, CB)], s_w.at[0, p])

    def load_wu(p):
        return pltpu.make_async_copy(w_up.at[ds(p, CB)], dwu.at[ds(p, CB)], s_w.at[1, p])

    def load_x(t):
        return pltpu.make_async_copy(x.at[:, ds(t, 256)], xv.at[rem(t, 2)], s_x.at[rem(t, 2)])

    def load_w(n):
        load_wg(n).start()
        load_wu(n).start()

    def load_rows(b):
        load_dy(b).start()
        load_g(b).start()
        load_u(b).start()

    load_wd(0).start()
    load_rows(0)
    load_wd(1).start()
    load_wd(2).start()
    load_w(0)

    barrier = pltpu.get_barrier_semaphore()
    for d in (sib, pair):
        pl.semaphore_signal(barrier, inc=1, device_id=(dp, d), device_id_type=MESH)

    @pl.when(mid)
    def _():
        pl.semaphore_signal(barrier, inc=1, device_id=(dp, across), device_id_type=MESH)


    def d_part(b, h):
        rows, cols = ds(b, RB), ds(h, 256)
        d_hidden = dot(dyv[rows, :], dwd[cols, :], NT)
        g = gv[rem(b, 2), :, cols].astype(F32)
        u = uv[rem(b, 2), :, cols].astype(F32)
        sig = jax.nn.sigmoid(g)
        act = g * sig
        hid[rows, cols] = (act * u).astype(BF16)
        dgu[rows, ds(HP + h, 256)] = (d_hidden * act).astype(BF16)
        dgu[rows, cols] = (d_hidden * u * (sig + act * (1.0 - sig))).astype(BF16)

    def term(k):
        rows, cols = ds(div(k, NC), RB), ds(rem(k, NC), CB)
        return dot(dgu[rows, :FF], dwg[cols, :], NT) + dot(dgu[rows, FF:], dwu[cols, :], NT)

    def remote(src, dst, send, recv, device):
        return pltpu.make_async_remote_copy(src, dst, send, recv, (dp, device), MESH)

    def tile(k):
        return ds(div(k, NC), RB), ds(rem(k, NC), CB)

    def spot(s):
        k, h = div(s, SUB), rem(s, SUB)
        return ds(div(k, NC) * SUB + h, PR_ROWS), ds(rem(k, NC), CB)

    def to_sib(k):
        q = rem(k, SLOTS)
        return remote(stage.at[q], dx.at[tile(k)], s_bs.at[q], s_br.at[k], sib)

    def to_mid(s):
        return remote(tb.at[s], tb.at[s], s_t, s_in.at[s], pair)

    def to_across(s):
        return remote(tb.at[s], tb.at[s], s_t, s_in.at[s], across)

    def part_to_sib(s):
        return remote(tb.at[s], dx.at[spot(s)], s_gs, s_pl.at[s], sib)

    def to_edge(s):
        ref = dx.at[spot(s)]
        return remote(ref, ref, s_f, s_in.at[s], pair)

    def final_to_sib(s):
        ref = dx.at[spot(s)]
        return remote(ref, ref, s_gs, s_gr, sib)

    def both(a, b):
        return pl.when(jnp.logical_and(a, b))

    def serve_a(k):
        @pl.when(adds)
        def _():
            to_sib(k).wait_recv()

        def total(h):
            rows, cols = spot(k * SUB + h)
            return own[rem(k, DEPTH), pl.ds(h * PR_ROWS, PR_ROWS), :] + dx[rows, cols].astype(F32)

        @both(adds, edge)
        def _():
            for h in range(SUB):
                s = k * SUB + h
                tb[s] = total(h).astype(BF16)
                to_mid(s).start()

        @both(adds, mid)
        def _():
            for h in range(SUB):
                own[rem(k, DEPTH), pl.ds(h * PR_ROWS, PR_ROWS), :] = total(h)

    def serve_p(s):
        @both(adds, mid)
        def _():
            to_mid(s).wait_recv()
            k, h = div(s, SUB), rem(s, SUB)
            tb[s] = (own[rem(k, DEPTH), ds(h, PR_ROWS), :] + tb[s].astype(F32)).astype(BF16)
            to_across(s).start()
            part_to_sib(s).start()

    def serve_f(s):
        @both(ends, mid)
        def _():
            part_to_sib(s).wait_recv()
            to_across(s).wait_recv()
            rows, cols = spot(s)
            dx[rows, cols] = (dx[rows, cols].astype(F32) + tb[s].astype(F32)).astype(BF16)
            to_edge(s).start()
            final_to_sib(s).start()

    def serve_g(s):
        @both(ends, edge)
        def _():
            to_edge(s).wait_recv()
            final_to_sib(s).start()

    def serve(i):
        for lag, f in ((LAG_P, serve_p), (LAG_F, serve_f), (LAG_G, serve_g)):
            s = i - lag
            pl.when(jnp.logical_and(s >= 0, s < PIECES))(functools.partial(f, s))

    load_dy(0).wait()
    load_g(0).wait()
    load_u(0).wait()
    for h in range(HP):
        load_wd(h).wait()
        if h == HP - 1:
            for n in range(1, NC):
                load_w(n)
            load_rows(1)
        d_part(0, h)

    @pl.when(edge)
    def _():
        pl.semaphore_wait(barrier, 2)

    @pl.when(mid)
    def _():
        pl.semaphore_wait(barrier, 3)

    def step1(i, _):
        b, n = div(i, NC), rem(i, NC)

        @pl.when(b == 0)
        def _():
            load_wg(n).wait()
            load_wu(n).wait()

        @both(ends, i >= SLOTS)
        def _():
            to_sib(i - SLOTS).wait_send()

        t = term(i)
        own[rem(i, DEPTH)] = t
        stage[rem(i, SLOTS)] = t.astype(BF16)

        @pl.when(ends)
        def _():
            to_sib(i).start()

        @pl.when(i >= 1)
        def _():
            serve_a(i - 1)

        serve(b * PER_BLOCK + n)

        @pl.when(jnp.logical_and(n == 1, b < NB - 1))
        def _():
            load_dy(b + 1).wait()
            load_g(b + 1).wait()
            load_u(b + 1).wait()

            @pl.when(b < NB - 2)
            def _():
                load_rows(b + 2)

        @pl.when(jnp.logical_and(n >= 1, b < NB - 1))
        def _():
            d_part(b + 1, n - 1)

        pl.when(n == NC - 1)(functools.partial(serve, b * PER_BLOCK + NC))

        @pl.when(i == CHUNKS - 2)
        def _():
            load_x(0).start()
            load_x(1).start()

        return 0

    lax.fori_loop(0, CHUNKS, step1, 0)
    serve_a(CHUNKS - 1)

    def step2(t, _):
        load_x(t).wait()
        rows = ds(t, 256)
        for q in range(3):
            part = dot(xv[rem(t, 2)], dgu[:, q * 512 : (q + 1) * 512], TN).astype(BF16)
            if q == 0:
                dwg[rows, :512] = part
            elif q == 1:
                dwg[rows, 512:] = part[:, :256]
                dwu[rows, :256] = part[:, 256:]
            else:
                dwu[rows, 256:] = part

                @pl.when(t < D // 256 - 2)
                def _():
                    load_x(t + 2).start()

            if q > 0:
                serve(NB * PER_BLOCK + 2 * t + q - 1)
        return 0

    lax.fori_loop(0, D // 256, step2, 0)
    base = NB * PER_BLOCK + 2 * (D // 256)

    def step3(i, _):
        q, h = div(i, HP), rem(i, HP)
        rows, cols = ds(h, 256), ds(q, 512)
        dwd[rows, cols] = dot(hid[:, rows], dyv[:, cols], TN).astype(BF16)
        pl.when(h > 0)(functools.partial(serve, base + q * (HP - 1) + h - 1))
        return 0

    lax.fori_loop(0, HP * 4, step3, 0)
    base = base + (HP - 1) * 4

    def step4(i, _):
        serve(i)
        return 0

    lax.fori_loop(base, PIECES + LAG_G, step4, 0)

    @pl.when(adds)
    def _():
        pltpu.make_async_copy(tb, tb, s_t).wait()
        pltpu.make_async_copy(dx, dx, s_gr).wait()

    @both(adds, mid)
    def _():
        pltpu.make_async_copy(tb, tb, s_gs).wait()

    @pl.when(ends)
    def _():
        for k in range(SLOTS):
            to_sib(CHUNKS - SLOTS + k).wait_send()
        pltpu.make_async_copy(dx, dx, s_gs).wait()

    @both(ends, mid)
    def _():
        pltpu.make_async_copy(dx, dx, s_f).wait()


def writer(a, b, c, d, oa, ob, oc, od, sems):
    copies = []
    for i, (src, dst) in enumerate(((a, oa), (b, ob), (c, oc), (d, od))):
        for k in range(4):
            rows = pl.ds(k * (src.shape[0] // 4), src.shape[0] // 4)
            copies.append(pltpu.make_async_copy(src.at[rows], dst.at[rows], sems.at[i, k]))
    for copy in copies:
        copy.start()
    for copy in copies:
        copy.wait()


def solution(mesh):
    shapes = ((ROWS, D), (D, FF), (D, FF), (FF, D))

    def step(*args):
        dma = pltpu.SemaphoreType.DMA
        parts = pl.pallas_call(
            kernel,
            out_shape=[pltpu.VMEM(s, BF16) for s in shapes],
            in_specs=[pl.BlockSpec(memory_space=pl.ANY)] * 7,
            out_specs=[pl.BlockSpec(memory_space=pltpu.VMEM)] * 4,
            scratch_shapes=[
                pltpu.VMEM((ROWS, D), BF16),
                pltpu.VMEM((ROWS, 2 * FF), BF16),
                pltpu.VMEM((ROWS, FF), BF16),
                pltpu.VMEM((DEPTH, RB, CB), F32),
                pltpu.VMEM((PIECES, PR_ROWS, CB), BF16),
                pltpu.VMEM((SLOTS, RB, CB), BF16),
                pltpu.VMEM((2, RB, FF), BF16),
                pltpu.VMEM((2, RB, FF), BF16),
                pltpu.VMEM((2, ROWS, 256), BF16),
                dma((NB,)),
                dma((2,)),
                dma((2,)),
                dma((2, NC)),
                dma((HP,)),
                dma((2,)),
                dma((SLOTS,)),
                dma((CHUNKS,)),
                dma,
                dma((PIECES,)),
                dma((PIECES,)),
                dma,
                dma,
                dma,
            ],
            compiler_params=pltpu.CompilerParams(
                collective_id=0, has_side_effects=True, vmem_limit_bytes=44 * 1024 * 1024
            ),
        )(*args)
        return pl.pallas_call(
            writer,
            out_shape=[jax.ShapeDtypeStruct(s, BF16) for s in shapes],
            in_specs=[pl.BlockSpec(memory_space=pltpu.VMEM)] * 4,
            out_specs=[pl.BlockSpec(memory_space=pl.ANY)] * 4,
            scratch_shapes=[pltpu.SemaphoreType.DMA((4, 4))],
            compiler_params=pltpu.CompilerParams(vmem_limit_bytes=1024 * 1024),
        )(*parts)

    tokens, columns, rows = P("dp", None), P(None, "tp"), P("tp", None)
    return jax.shard_map(
        step,
        mesh=mesh,
        in_specs=(tokens, tokens, P("dp", "tp"), P("dp", "tp"), columns, columns, rows),
        out_specs=(tokens, P("dp", "tp"), P("dp", "tp"), P(("dp", "tp"), None)),
        check_vma=False,
    )
```
